32 devices in a mesh: lat: 16 (over z, y, core), ma: 2 (over x).
Axes of the slice: x: 2, y: 2, z: 4, core: 2. Of those that a mesh axis runs over, the one named last changes fastest.
Arguments:
- pair_wave: int32 [360], replicated, may hold values from 0 to 359, each once
- legendre: bfloat16 [360, 160, 736], P('ma', 'lat'), may hold values from -0.0078125 to 0.0078125
- coefs: bfloat16 [360, 736, 168], P('ma', 'lat'), may hold values from -6 to 6
Outputs:
- noise: float32 [13440, 1440], P(('lat', 'ma'))
The draws below stay inside these ranges and needn't reach their ends.
Inputs may be any that keep to these rules, and one draw needn't show every extreme that they name: Slot q holds wavenumbers pair_wave[q] and 719 - pair_wave[q]; every value appears once.
All inputs are finite; a program needn't handle non-finite values.
Results may differ from the reference program's by a relative error of at most 0.0003.
Values may be sent and summed in bfloat16 or wider, within the bound.
A program may use at most 64 MiB of HBM per device.

```python
import math
import jax
import jax.numpy as jnp
from jax import lax

DEG = 720
LON = 1440
CH = 84
LAT_DEV = 10
PAIRS = 360
RROWS = 736
COLS = 168
LATS = 160
N_LAT = 16
N_MA = 2


def level_of(key, dims, split, smallest, high):
    factor_of = 1.0
    for axis_at, shards_of in split:
        draws = jax.random.uniform(jax.random.fold_in(jax.random.fold_in(key, 6), axis_at), (shards_of,), jnp.float32, smallest / len(split), high / len(split))
        factor_of = factor_of * jnp.repeat(jnp.exp(draws), dims[axis_at] // shards_of).reshape((-1,) + (1,) * (len(dims) - 1 - axis_at))
    return factor_of


def noise(stream_key, extent, deviation, most, shards=(), kind=jnp.bfloat16):
    values = jax.random.normal(stream_key, extent, jnp.float32) * deviation
    if len(shards) > 0:
        values = level_of(stream_key, extent, shards, -0.22, 0.18) * values
    return jnp.clip(values, min=-most, max=most).astype(kind)


def setup_inputs(seed: int = 0) -> dict:
    key_list = jax.random.split(jax.random.key(seed), 4)
    pair_wave = jax.random.permutation(key_list[0], PAIRS).astype(jnp.int32)
    legendre = noise(key_list[1], (PAIRS, LATS, RROWS), (RROWS * DEG) ** -0.5, 0.0078125, ((0, 2), (1, 16)))
    coefs = noise(key_list[2], (PAIRS, RROWS, COLS), 1.0, 6.0, ((0, 2), (1, 16)))
    return dict(pair_wave=pair_wave, legendre=legendre, coefs=coefs)


def chain_table(table, wave_ids, degree_top):
    row_count = table.shape[2]
    row_ids = jnp.arange(row_count, dtype=jnp.int32)[None, :]
    split_row = (degree_top - wave_ids).astype(jnp.int32)[:, None]
    inside = row_ids < split_row
    outside = (row_ids >= split_row) & (row_ids <= degree_top)
    masks = jnp.stack([inside, outside], axis=1)
    return jnp.where(masks[:, :, None, :], table[:, None, :, :], jnp.zeros((), table.dtype))


def fourier_basis(pair_wave, degree_top, lon_count):
    orders = jnp.stack([pair_wave, degree_top - 1 - pair_wave], axis=1).astype(jnp.int32)
    positions = jnp.arange(lon_count, dtype=jnp.int32)
    phase_int = (orders[:, :, None] * positions[None, None, :]) % lon_count
    radians = (2.0 * math.pi / lon_count) * phase_int.astype(jnp.float32)
    weight = jnp.where(orders == 0, 1.0, 2.0).astype(jnp.float32)[:, :, None]
    real_row = weight * jnp.cos(radians)
    imag_row = -weight * jnp.sin(radians)
    return jnp.stack([real_row, imag_row], axis=2).reshape(-1, lon_count)


def reference(pair_wave, legendre, coefs):
    pair_count = pair_wave.shape[0]
    row_count = coefs.shape[1]
    lat_total = LAT_DEV * N_LAT
    slot_count = pair_count // N_MA

    def group_spectra(packed):
        wave_ids, group_table, group_coefs = packed
        masked = chain_table(group_table, wave_ids, DEG)
        return jnp.einsum('qeir,qrc->qeic', masked.astype(jnp.float32), group_coefs.astype(jnp.float32), precision=lax.Precision.HIGHEST)

    spectra = lax.map(group_spectra, (pair_wave.reshape(N_MA, slot_count), legendre.reshape(N_MA, slot_count, lat_total, row_count), coefs.reshape(N_MA, slot_count, row_count, coefs.shape[2])))
    spectra = spectra.reshape(pair_count, 2, lat_total, 2, CH)
    fourier_rows = jnp.transpose(spectra, (0, 1, 3, 2, 4)).reshape(4 * pair_count, lat_total * CH)
    synth_basis = fourier_basis(pair_wave, DEG, LON)
    return lax.dot_general(fourier_rows, synth_basis, (((0,), (0,)), ((), ())), precision=lax.Precision.HIGHEST)
```

```python
import math

import jax
import jax.numpy as jnp
from jax import lax
from jax.sharding import PartitionSpec as P

LON = 1440


def split_bf16(x):
    hi = lax.reduce_precision(x, 8, 7)
    return hi.astype(jnp.bfloat16), (x - hi).astype(jnp.bfloat16)


def basis_rows(waves, quarter, lon_count):
    positions = jnp.arange(lon_count, dtype=jnp.int32)
    phase = (waves[:, None] * positions[None, :] + quarter[:, None]) % lon_count
    radians = 2.0 * math.pi / lon_count * phase.astype(jnp.float32)
    weight = jnp.where(waves == 0, 1.0, 2.0).astype(jnp.float32)[:, None]
    return split_bf16(weight * jnp.cos(radians))


def dot_rows(rows, basis):
    return lax.dot_general(
        rows, basis, (((0,), (0,)), ((), ())), preferred_element_type=jnp.float32
    )


def body(pair_wave, legendre, coefs):
    lat_n = lax.axis_size("lat")
    ma_n = lax.axis_size("ma")
    lat_i = lax.axis_index("lat")
    ma_i = lax.axis_index("ma")
    slots, rows_dev, row_count = legendre.shape
    deg_dev, cols = coefs.shape[1:]
    ch = cols // 2
    degree_top = 2 * pair_wave.shape[0]
    per = -(-slots // lat_n)
    per += -per % 2
    padded = per * lat_n
    waves = jnp.pad(pair_wave.reshape(ma_n, slots), ((0, 0), (0, padded - slots)))
    waves = waves.reshape(ma_n, lat_n, per)

    order = waves.transpose(1, 0, 2).reshape(-1, 1, 1, per)
    order = jnp.concatenate([order, degree_top - 1 - order], axis=2)
    order = jnp.broadcast_to(order, (lat_n * ma_n, 2, 2, per))
    quarter = jnp.arange(2, dtype=jnp.int32)[None, :, None, None] * (LON // 4)
    quarter = jnp.broadcast_to(quarter, order.shape)
    b_hi, b_lo = basis_rows(order.reshape(-1), quarter.reshape(-1), LON)

    table = jnp.transpose(legendre, (1, 0, 2))
    table = jnp.pad(table, ((0, 0), (0, padded - slots), (0, 0)))
    table = table.reshape(rows_dev, lat_n, per, row_count).transpose(1, 0, 2, 3)
    table = table.reshape(lat_n, rows_dev * per, row_count)
    table = lax.all_to_all(table, "lat", split_axis=0, concat_axis=0, tiled=True)
    table = table.reshape(lat_n * rows_dev, per, row_count).transpose(1, 0, 2)

    full = cols // 128 * 128
    rest = cols - full
    group = 1
    for g in range(1, 128 // rest + 1):
        if per % g == 0:
            group = g
    packed = jnp.pad(coefs, ((0, padded - slots), (0, 0), (0, 0)))
    packed = packed.reshape(lat_n, per, deg_dev, cols)
    head = packed[..., :full].reshape(lat_n, per * deg_dev, full)
    tail = packed[..., full:].reshape(lat_n, group, per // group, deg_dev, rest)
    tail = jnp.concatenate([tail[:, g] for g in range(group)], axis=-1)
    tail = tail.reshape(lat_n, per // group * deg_dev, group * rest)
    tail = jnp.pad(tail, ((0, 0), (0, 0), (0, 128 - group * rest)))
    both = jnp.concatenate([head, tail], axis=1)
    both = lax.all_to_all(both, "lat", split_axis=0, concat_axis=0, tiled=True)
    both, b_hi, b_lo = lax.optimization_barrier((both, b_hi, b_lo))
    head = both[:, : per * deg_dev].reshape(lat_n, per, deg_dev, full)
    tail = both[:, per * deg_dev :].reshape(lat_n, per // group, deg_dev, 128)
    tail = jnp.concatenate(
        [tail[..., g * rest : (g + 1) * rest] for g in range(group)], axis=1
    )
    mine = jnp.concatenate([head, tail], axis=-1)
    mine = mine.transpose(1, 0, 2, 3).reshape(per, row_count, cols)

    my_waves = waves[ma_i, lat_i]
    row_ids = jnp.arange(row_count, dtype=jnp.int32)[None, :]
    split_row = (degree_top - my_waves)[:, None]
    inside = row_ids < split_row
    outside = (row_ids >= split_row) & (row_ids <= degree_top)
    masks = jnp.stack([inside, outside], axis=1)
    masked = jnp.where(masks[:, :, None, :], table[:, None], jnp.zeros((), table.dtype))
    sums = jnp.einsum("qhir,qrc->qhic", masked, mine, preferred_element_type=jnp.float32)

    places = lat_n * ma_n
    width = rows_dev * ch // ma_n
    sums = sums.reshape(per, 2, lat_n, rows_dev, 2, ch).transpose(2, 4, 1, 0, 3, 5)
    sums = sums.reshape(lat_n, 4 * per, ma_n, width).transpose(0, 2, 1, 3)
    top = jnp.max(jnp.abs(sums), axis=3, keepdims=True)
    power = jnp.ceil(jnp.log2(jnp.maximum(top, 1e-30)) + 1e-3)
    coded = jnp.round(sums * (jnp.exp2(-power) * 32767.0)).astype(jnp.int16)
    coded = jnp.concatenate([coded, power.astype(jnp.int16)], axis=3)
    coded = coded.reshape(places, 4 * per, width + 1)
    coded = lax.all_to_all(coded, ("lat", "ma"), split_axis=0, concat_axis=0, tiled=True)
    spectra = coded[..., :width].astype(jnp.float32)
    scale = jnp.exp2(coded[..., width:].astype(jnp.float32)) * (1.0 / 32767.0)
    spectra = (spectra * scale).reshape(places * 4 * per, width)
    f_hi, f_lo = split_bf16(spectra)
    return dot_rows(f_hi, b_hi) + (dot_rows(f_hi, b_lo) + dot_rows(f_lo, b_hi))


def solution(mesh):
    in_specs = (P(), P("ma", "lat", None), P("ma", "lat", None))
    out_specs = P(("lat", "ma"), None)
    return jax.shard_map(body, mesh=mesh, in_specs=in_specs, out_specs=out_specs, check_vma=False)
```

```python
import math

import jax
import jax.numpy as jnp
from jax import lax
from jax.sharding import PartitionSpec as P

LON = 1440
SINE = [(-1.0) ** n / math.factorial(2 * n + 1) for n in range(7)]


def split_bf16(x):
    hi = lax.reduce_precision(x, 8, 7)
    return hi.astype(jnp.bfloat16), (x - hi).astype(jnp.bfloat16)


def basis_rows(waves, quarter, lon_count):
    positions = jnp.arange(lon_count, dtype=jnp.int32).astype(jnp.float32)
    order = waves.astype(jnp.float32)
    phase = order[:, None] * positions[None, :] + quarter.astype(jnp.float32)[:, None]
    turns = jnp.round(phase * (1.0 / lon_count))
    angle = (phase - turns * lon_count) * (math.pi / lon_count)
    square = angle * angle
    poly = jnp.float32(SINE[-1])
    for coefficient in SINE[-2::-1]:
        poly = poly * square + coefficient
    sine = angle * poly
    weight = jnp.where(waves == 0, 1.0, 2.0).astype(jnp.float32)[:, None]
    return split_bf16(weight - (2.0 * weight) * (sine * sine))


def dot_rows(rows, basis):
    return lax.dot_general(
        rows, basis, (((0,), (0,)), ((), ())), preferred_element_type=jnp.float32
    )


def lay_out(waves, chunks, lat_n):
    parts = []
    start = 0
    for size in chunks:
        stop = start + size * lat_n
        part = waves[:, start : min(stop, waves.shape[1])]
        part = jnp.pad(part, ((0, 0), (0, size * lat_n - part.shape[1])))
        parts.append(part.reshape(-1, lat_n, size))
        start = stop
    return parts


def take_slots(x, axis, start, size):
    stop = min(start + size, x.shape[axis])
    x = lax.slice_in_dim(x, start, stop, axis=axis)
    pads = [(0, 0)] * x.ndim
    pads[axis] = (0, size - (stop - start))
    return jnp.pad(x, pads)


def send_table(legendre, start, size, lat_n):
    rows_dev, _, row_count = legendre.shape
    table = take_slots(legendre, 1, start, size * lat_n)
    table = table.reshape(rows_dev, lat_n, size, row_count).transpose(1, 0, 2, 3)
    return table.reshape(lat_n, rows_dev * size, row_count)


def pack_coefs(coefs, start, size, lat_n, full, group):
    _, deg_dev, cols = coefs.shape
    rest = cols - full
    block = -(-deg_dev // group)
    packed = take_slots(coefs, 0, start, size * lat_n)
    head = packed[..., :full]
    tail = jnp.pad(packed[..., full:], ((0, 0), (0, block * group - deg_dev), (0, 0)))
    tail = jnp.concatenate(
        [tail[:, g * block : (g + 1) * block] for g in range(group)], axis=-1
    )
    tail = jnp.pad(tail, ((0, 0), (0, 0), (0, 128 - group * rest)))
    head = jnp.pad(head, ((0, 0), (0, -deg_dev % 16), (0, 0)))
    both = jnp.concatenate([head, tail], axis=1)
    return both.reshape(lat_n, -1, 128)


def unpack_coefs(both, size, deg_dev, rest, group):
    lat_n = both.shape[0]
    block = -(-deg_dev // group)
    both = both.reshape(lat_n, size, -1, 128)
    head = both[:, :, :deg_dev]
    tail = both[:, :, deg_dev + -deg_dev % 16 :]
    tail = jnp.concatenate(
        [tail[..., g * rest : (g + 1) * rest] for g in range(group)], axis=2
    )
    mine = jnp.concatenate([head, tail[:, :, :deg_dev]], axis=-1)
    return mine.transpose(1, 0, 2, 3).reshape(size, lat_n * deg_dev, -1)


def slot_sums(table, mine, waves, degree_top):
    row_ids = jnp.arange(table.shape[2], dtype=jnp.int32)[None, :]
    split_row = (degree_top - waves)[:, None]
    inside = row_ids < split_row
    outside = (row_ids >= split_row) & (row_ids <= degree_top)
    masks = jnp.stack([inside, outside], axis=1)
    masked = jnp.where(masks[:, :, None, :], table[:, None], jnp.zeros((), table.dtype))
    return jnp.einsum("qhir,qrc->qhic", masked, mine, preferred_element_type=jnp.float32)


def code_rows(sums, lat_n, ma_n):
    size, _, lats, cols = sums.shape
    rows_dev, ch = lats // lat_n, cols // 2
    width = rows_dev * ch // ma_n
    sums = sums.reshape(size, 2, lat_n, rows_dev, 2, ch).transpose(2, 0, 1, 4, 3, 5)
    sums = sums.reshape(lat_n, 2 * size, 2, ma_n, width).transpose(0, 3, 1, 2, 4)
    top = jnp.max(jnp.abs(sums), axis=4, keepdims=True)
    power = jnp.ceil(jnp.log2(jnp.maximum(top, 1e-30)) + 1e-3)
    coded = jnp.round(sums * (jnp.exp2(-power) * 32767.0)).astype(jnp.int16)
    coded = coded.reshape(lat_n * ma_n, 2 * size, 2 * width)
    power = power.astype(jnp.int16).reshape(lat_n * ma_n, 2 * size, 2)
    return jnp.concatenate([coded, power], axis=2)


def decode_rows(coded):
    width = coded.shape[2] // 2 - 1
    halves = []
    for e in range(2):
        part = coded[..., e * width : (e + 1) * width].astype(jnp.float32)
        power = coded[..., 2 * width + e : 2 * width + e + 1].astype(jnp.float32)
        part = part * (jnp.exp2(power) * (1.0 / 32767.0))
        halves.append(split_bf16(part.reshape(-1, width)))
    return halves


def exchange(x, axes):
    return lax.all_to_all(x, axes, split_axis=0, concat_axis=0, tiled=True)


def chunk_basis(part, degree_top):
    order = part.transpose(1, 0, 2).reshape(-1, 1)
    order = jnp.concatenate([order, degree_top - 1 - order], axis=1).reshape(-1)
    quarter = jnp.full_like(order, LON // 4)
    return [basis_rows(order, e * quarter, LON) for e in range(2)]


def body(pair_wave, legendre, coefs):
    lat_n = lax.axis_size("lat")
    ma_n = lax.axis_size("ma")
    lat_i = lax.axis_index("lat")
    ma_i = lax.axis_index("ma")
    slots, rows_dev, row_count = legendre.shape
    deg_dev, cols = coefs.shape[1:]
    degree_top = 2 * pair_wave.shape[0]
    per = -(-slots // lat_n)
    per += -per % 4 if per > 4 else per % 2
    chunks = [per - 4, 4] if per > 4 else [per]
    full = cols // 128 * 128
    rest = cols - full
    group = min(128 // rest, deg_dev)
    parts = lay_out(pair_wave.reshape(ma_n, slots), chunks, lat_n)
    legendre = jnp.transpose(legendre, (1, 0, 2))

    def make_coded(pair, size, part):
        table, both = pair
        mine = unpack_coefs(both, size, deg_dev, rest, group)
        sums = slot_sums(table, mine, part[ma_i, lat_i], degree_top)
        return code_rows(sums, lat_n, ma_n)

    coded_list = []
    ready = None
    arrived = []
    bases = [chunk_basis(part, degree_top) for part in parts]
    tables = []
    packs = []
    start = 0
    for size in chunks:
        tables.append(send_table(legendre, start, size, lat_n))
        packs.append(pack_coefs(coefs, start, size, lat_n, full, group))
        start += size * lat_n
    table = exchange(jnp.concatenate(tables, axis=1), "lat")
    table, packs, bases = lax.optimization_barrier((table, packs, bases))
    offset = 0
    for k, size in enumerate(chunks):
        both = packs[k]
        if k > 0:
            both, ready = lax.optimization_barrier((both, ready))
        both = exchange(both, "lat")
        ready = both
        if k > 0:
            prev = make_coded(arrived[-1], chunks[k - 1], parts[k - 1])
            both, prev = lax.optimization_barrier((both, prev))
            coded_list.append(prev)
        piece = table[:, offset : offset + rows_dev * size]
        piece = piece.reshape(lat_n * rows_dev, size, row_count).transpose(1, 0, 2)
        both, piece = lax.optimization_barrier((both, piece))
        arrived.append((piece, both))
        offset += rows_dev * size

    if len(chunks) == 1:
        last = make_coded(arrived[-1], chunks[-1], parts[-1])
    total = None
    for k, basis in enumerate(bases):
        coded = exchange(coded_list[k] if k < len(coded_list) else last, ("lat", "ma"))
        if k == len(bases) - 2:
            last = make_coded(arrived[-1], chunks[-1], parts[-1])
            coded, last = lax.optimization_barrier((coded, last))
        for (f_hi, f_lo), (b_hi, b_lo) in zip(decode_rows(coded), basis):
            term = dot_rows(f_hi, b_hi) + (dot_rows(f_hi, b_lo) + dot_rows(f_lo, b_hi))
            total = term if total is None else total + term
    return total


def solution(mesh):
    in_specs = (P(), P("ma", "lat", None), P("ma", "lat", None))
    out_specs = P(("lat", "ma"), None)
    return jax.shard_map(body, mesh=mesh, in_specs=in_specs, out_specs=out_specs, check_vma=False)
```
